256 devices in a mesh: blk: 32 (over x, z), src: 2 (over y_lo), layer: 4 (over y_hi, core).
Axes of the slice: x: 4, y: 4 (y_hi: 2, y_lo: 2; y = y_hi * 2 + y_lo), z: 8, core: 2. Of those that a mesh axis runs over, the one named last changes fastest.
Arguments:
- resident_act: bfloat16 [4, 16384, 4096], P('layer', 'blk'), may hold values from -6 to 6
- resident_grad: bfloat16 [4, 16384, 4096], P('layer', 'blk'), may hold values from -6 to 6
- source_act: bfloat16 [4, 1024, 4096], P('layer', ('blk', 'src')), may hold values from -6 to 6
- source_grad: bfloat16 [4, 1024, 4096], P('layer', ('blk', 'src')), may hold values from -6 to 6
- probes: bfloat16 [1024, 256], P(('blk', 'src')), may hold values from -6 to 6
Outputs:
- kernel_product: float32 [16384, 256], P(('blk', 'layer'))
The draws below stay inside these ranges and needn't reach their ends.
All inputs are finite; a program needn't handle non-finite values.
Results may differ from the reference program's by a relative error of at most 0.0029.
Values may be sent and summed in bfloat16 or wider, within the bound.
No kernel may reach another device: no remote copies, remote signals or barrier semaphores. Data moves between devices by JAX's collectives and lax.ppermute only.
A program may use at most 64 MiB of HBM per device.

```python
import jax
import jax.numpy as jnp
from jax import lax

D = 4096
PROBE = 256
LAYERS = 4
RES = 16384
SOURCE = 1024


def shard_levels(rng, shape, cuts, smallest, high):
    def one(position, shards_of):
        steps = jax.random.uniform(jax.random.fold_in(jax.random.fold_in(rng, 6), position), (shards_of,), jnp.float32, smallest / len(cuts), high / len(cuts))
        return jnp.repeat(jnp.exp(steps), shape[position] // shards_of).reshape((-1,) + (1,) * (len(shape) - position - 1))

    level = one(*cuts[0])
    for cut in cuts[1:]:
        level = level * one(*cut)
    return level


def bell_draw(key, shape, spread, reach, shards=(), held_as=jnp.bfloat16):
    drawn = spread * jax.random.normal(key, shape, jnp.float32)
    if shards:
        drawn = drawn * shard_levels(key, shape, shards, -0.22, 0.18)
    return jnp.clip(drawn, -reach, reach).astype(held_as)


def setup_inputs(seed: int = 0) -> dict:
    seeds = jax.random.split(jax.random.key(seed), 6)
    resident_act = bell_draw(seeds[0], (LAYERS, RES, D), 1.0, 6.0, ((0, 4), (1, 32)))
    resident_grad = bell_draw(seeds[1], (LAYERS, RES, D), 1.0, 6.0, ((0, 4), (1, 32)))
    source_act = bell_draw(seeds[2], (LAYERS, SOURCE, D), 1.0, 6.0, ((0, 4), (1, 64)))
    source_grad = bell_draw(seeds[3], (LAYERS, SOURCE, D), 1.0, 6.0, ((0, 4), (1, 64)))
    probes = bell_draw(seeds[4], (SOURCE, PROBE), 1.0, 6.0, ((0, 64),))
    return {"resident_act": resident_act, "resident_grad": resident_grad, "source_act": source_act, "source_grad": source_grad, "probes": probes}


def reference(resident_act, resident_grad, source_act, source_grad, probes):
    def one_layer(total, items):
        res_a, res_g, src_a, src_g = items
        act_gram = jnp.dot(src_a, res_a.T, preferred_element_type=jnp.float32)
        grad_gram = jnp.dot(src_g, res_g.T, preferred_element_type=jnp.float32)
        kernel = (act_gram * grad_gram * jnp.float32(1.0 / D)).astype(jnp.bfloat16)
        total = total + jnp.dot(kernel.T, probes, preferred_element_type=jnp.float32)
        return total, None

    start = jnp.zeros((RES, PROBE), jnp.float32)
    total, _ = lax.scan(one_layer, start, (resident_act, resident_grad, source_act, source_grad))
    return total * jnp.float32((LAYERS * SOURCE) ** -0.5)
```

```python
import jax
import jax.numpy as jnp
from jax import lax
from jax.sharding import PartitionSpec as P

LAYERS = 4


def contract_rows(left, right):
    return lax.dot_general(
        left, right, (((1,), (1,)), ((), ())), preferred_element_type=jnp.float32
    )


def on_device(resident_act, resident_grad, source_act, source_grad, probes):
    width = resident_act.shape[2]
    blocks = lax.axis_size("blk")
    source_total = source_act.shape[1] * blocks * lax.axis_size("src")
    inverse_width = jnp.float32(1.0 / width)

    probe_rows = lax.all_gather(probes, "blk", axis=0, tiled=True)
    acts = lax.all_gather(source_act[0], "blk", axis=0, tiled=True)
    grads = lax.all_gather(source_grad[0], "blk", axis=0, tiled=True)
    act_gram = contract_rows(acts, resident_act[0])
    grad_gram = contract_rows(grads, resident_grad[0])
    kernel = (act_gram * grad_gram * inverse_width).astype(jnp.bfloat16)
    total = lax.dot_general(
        kernel, probe_rows, (((0,), (0,)), ((), ())), preferred_element_type=jnp.float32
    )
    part = lax.psum_scatter(total, "layer", scatter_dimension=0, tiled=True)
    result = lax.psum(part, "src")
    return result * jnp.float32((LAYERS * source_total) ** (-0.5))


def solution(mesh):
    in_specs = (
        P("layer", "blk", None),
        P("layer", "blk", None),
        P("layer", ("blk", "src"), None),
        P("layer", ("blk", "src"), None),
        P(("blk", "src"), None),
    )
    out_specs = P(("blk", "layer"), None)
    return jax.shard_map(
        on_device, mesh=mesh, in_specs=in_specs, out_specs=out_specs, check_vma=False
    )
```

```python
import functools

import jax
import jax.numpy as jnp
from jax import lax
from jax.experimental import pallas as pl
from jax.experimental.pallas import tpu as pltpu
from jax.sharding import PartitionSpec as P


LAYERS = 4
ACROSS, ALONG = 4, 8
HOPS = {"zp": (0, 1), "zm": (0, -1), "xp": (1, 0), "xm": (-1, 0)}
ROUTE = (
    ("zp", (0, 0)),
    ("xp", (0, 0)),
    ("xm", (0, 0)),
    ("zm", (0, 0)),
    ("zp", (0, 1)),
    ("xp", (1, 0)),
    ("xm", (0, 1)),
    ("zm", (0, 7)),
    ("zp", (1, 0)),
    ("xp", (0, 7)),
    ("xm", (0, 2)),
    ("zm", (2, 0)),
    ("zp", (2, 0)),
    ("xp", (0, 6)),
    ("xm", (0, 6)),
    ("zm", (0, 6)),
    ("zp", (3, 2)),
    ("xp", (0, 2)),
    ("xm", (3, 2)),
    ("zm", (1, 6)),
    ("zp", (0, 2)),
    ("xp", (1, 6)),
    ("xm", (3, 3)),
    ("zm", (0, 5)),
    ("zp", (3, 3)),
    ("xp", (1, 5)),
    ("xm", (0, 5)),
    ("zm", (1, 5)),
    ("zp", (2, 3)),
    ("xp", (0, 3)),
    ("xm", (0, 7)),
)
CHUNKS = (16, 8, 8)


def hop_pairs(hop):
    dx, dz = HOPS[hop]
    return [
        (x * ALONG + z, (x + dx) % ACROSS * ALONG + (z + dz) % ALONG)
        for x in range(ACROSS)
        for z in range(ALONG)
    ]


def moved(offset, hop):
    dx, dz = HOPS[hop]
    return ((offset[0] + dx) % ACROSS, (offset[1] + dz) % ALONG)


def chunk_kernel(count, width, inverse_width, first, *refs):
    res_act, res_grad = refs[:2]
    blocks = refs[2 : 2 + count]
    rest = refs[2 + count :]
    if first:
        out, rows = rest
    else:
        before, out, rows = rest
    depth = blocks[0].shape[0]
    for i, block in enumerate(blocks):
        rows[i * depth : (i + 1) * depth, :] = block[...]

    def contract(left, right):
        return lax.dot_general(
            left, right, (((1,), (1,)), ((), ())), preferred_element_type=jnp.float32
        )

    act_gram = contract(res_act[...], rows[:, :width])
    grad_gram = contract(res_grad[...], rows[:, width : 2 * width])
    kernel = (act_gram * grad_gram * inverse_width).astype(jnp.bfloat16)
    part = jnp.dot(kernel, rows[:, 2 * width :], preferred_element_type=jnp.float32)
    if first:
        out[...] = part
    else:
        out[...] = before[...] + part


def add_chunk(total, res_act, res_grad, blocks):
    width = res_act.shape[1]
    first = total is None
    operands = [res_act, res_grad, *blocks] + ([] if first else [total])
    depth, wide = blocks[0].shape
    out = jax.ShapeDtypeStruct((res_act.shape[0], wide - 2 * width), jnp.float32)
    flops = 4 * res_act.shape[0] * width * depth * len(blocks)
    return pl.pallas_call(
        functools.partial(chunk_kernel, len(blocks), width, 1.0 / width, first),
        out_shape=out,
        in_specs=[pl.BlockSpec(memory_space=pltpu.VMEM)] * len(operands),
        out_specs=pl.BlockSpec(memory_space=pltpu.VMEM),
        scratch_shapes=[pltpu.VMEM((depth * len(blocks), wide), blocks[0].dtype)],
        compiler_params=pltpu.CompilerParams(vmem_limit_bytes=16 << 20),
        cost_estimate=pl.CostEstimate(flops=flops, bytes_accessed=0, transcendentals=0),
    )(*operands)


def on_device(resident_act, resident_grad, source_act, source_grad, probes):
    blocks = lax.axis_size("blk")
    source_total = source_act.shape[1] * blocks * lax.axis_size("src")
    res_act, res_grad = resident_act[0], resident_grad[0]

    own = jnp.concatenate([source_act[0], source_grad[0], probes], axis=1)
    held = {(0, 0): own}
    order = [(0, 0)]
    for hop, offset in ROUTE:
        there = moved(offset, hop)
        held[there] = lax.ppermute(held[offset], "blk", hop_pairs(hop))
        order.append(there)
    total = None
    begin = 0
    for size in CHUNKS:
        total = add_chunk(total, res_act, res_grad, [held[o] for o in order[begin : begin + size]])
        begin += size

    layer = lax.axis_index("layer")
    core, high = layer % 2, layer // 2
    pieces = total.reshape(2, 2, -1, total.shape[1])
    keep = lax.dynamic_index_in_dim(pieces, core, 1, keepdims=False)
    give = lax.dynamic_index_in_dim(pieces, 1 - core, 1, keepdims=False)
    chip = keep + lax.ppermute(give, "layer", [(l, l ^ 1) for l in range(LAYERS)])
    mine = lax.dynamic_index_in_dim(chip, high, 0, keepdims=False)
    other = lax.dynamic_index_in_dim(chip, 1 - high, 0, keepdims=False)

    def exchange(value, flip_src, flip_high):
        pairs = [
            (s * LAYERS + l, (s ^ flip_src) * LAYERS + (l ^ (2 * flip_high)))
            for s in range(2)
            for l in range(LAYERS)
        ]
        return lax.ppermute(value, ("src", "layer"), pairs)

    far = exchange(other, 0, 1)
    near = exchange(mine, 1, 0)
    wrap = exchange(other, 1, 1)
    result = mine + near + wrap + far
    return result * jnp.float32((LAYERS * source_total) ** (-0.5))


def solution(mesh):
    in_specs = (
        P("layer", "blk", None),
        P("layer", "blk", None),
        P("layer", ("blk", "src"), None),
        P("layer", ("blk", "src"), None),
        P(("blk", "src"), None),
    )
    out_specs = P(("blk", "layer"), None)
    return jax.shard_map(
        on_device, mesh=mesh, in_specs=in_specs, out_specs=out_specs, check_vma=False
    )
```

```python
import functools

import jax
import jax.numpy as jnp
from jax import lax
from jax.experimental import pallas as pl
from jax.experimental.pallas import tpu as pltpu
from jax.sharding import PartitionSpec as P


LAYERS = 4
ACROSS, ALONG = 4, 8
HOPS = {"zp": (0, 1), "zm": (0, -1), "xp": (1, 0), "xm": (-1, 0)}
ROUTE = (
    ("zm", (0, 0)),
    ("zp", (0, 0)),
    ("xm", (0, 0)),
    ("xp", (0, 0)),
    ("zm", (0, 7)),
    ("zp", (0, 1)),
    ("xp", (0, 1)),
    ("xm", (3, 0)),
    ("zm", (3, 0)),
    ("xm", (0, 1)),
    ("xp", (0, 6)),
    ("zm", (0, 6)),
    ("zp", (0, 2)),
    ("zp", (1, 1)),
    ("xp", (1, 1)),
    ("xm", (0, 6)),
    ("zm", (1, 6)),
    ("xm", (0, 2)),
    ("xp", (1, 6)),
    ("xp", (0, 7)),
    ("xp", (0, 3)),
    ("xm", (0, 3)),
    ("zm", (0, 5)),
    ("zp", (2, 1)),
    ("zm", (1, 5)),
    ("zm", (2, 6)),
    ("zp", (2, 6)),
    ("xm", (0, 5)),
    ("zp", (3, 3)),
    ("xm", (3, 3)),
    ("xp", (1, 4)),
)
CHUNKS = (16, 16)
TOUCH_AFTER = (4, 10, 16, 22, 31)


def hop_pairs(hop):
    dx, dz = HOPS[hop]
    return [
        (x * ALONG + z, (x + dx) % ACROSS * ALONG + (z + dz) % ALONG)
        for x in range(ACROSS)
        for z in range(ALONG)
    ]


def moved(offset, hop):
    dx, dz = HOPS[hop]
    return ((offset[0] + dx) % ACROSS, (offset[1] + dz) % ALONG)


STEP = 1024


def contract(left, right):
    return lax.dot_general(
        left, right, (((1,), (1,)), ((), ())), preferred_element_type=jnp.float32
    )


def chunk_kernel(count, width, inverse_width, first, tag, *refs):
    residents = refs[:2]
    blocks = refs[2 : 2 + count]
    rest = refs[2 + count :]

    def columns(begin, end):
        return jnp.concatenate([block[:, begin:end] for block in blocks], axis=0)

    grams = []
    for tensor, resident in enumerate(residents):
        gram = None
        for begin in range(0, width, STEP):
            base = tensor * width + begin
            piece = contract(resident[:, begin : begin + STEP], columns(base, base + STEP))
            gram = piece if gram is None else gram + piece
        grams.append(gram)
    kernel = (grams[0] * grams[1] * inverse_width).astype(jnp.bfloat16)
    rows = columns(2 * width, blocks[0].shape[1])
    part = jnp.dot(kernel, rows, preferred_element_type=jnp.float32)
    if first:
        rest[0][...] = part
    else:
        rest[1][...] = rest[0][...] + part


def touch_kernel(act, grad, *refs):
    out = refs[-1]
    out[...] = act[:16, :128] + grad[:16, :128]


def touch(act, grad, tag):
    in_vmem = pl.BlockSpec(memory_space=pltpu.VMEM)
    operands = [act, grad] + ([] if tag is None else [tag])
    return pl.pallas_call(
        touch_kernel,
        out_shape=jax.ShapeDtypeStruct((16, 128), act.dtype),
        in_specs=[in_vmem] * len(operands),
        out_specs=in_vmem,
        compiler_params=pltpu.CompilerParams(vmem_limit_bytes=1 << 20),
        cost_estimate=pl.CostEstimate(flops=1, bytes_accessed=1, transcendentals=0),
    )(*operands)


def add_chunk(total, tag, res_act, res_grad, blocks):
    width = res_act.shape[1]
    first = total is None
    operands = [tag, res_act, res_grad, *blocks] + ([] if first else [total])
    _, wide = blocks[0].shape
    out = jax.ShapeDtypeStruct((res_act.shape[0], wide - 2 * width), jnp.float32)
    return pl.pallas_call(
        functools.partial(chunk_kernel, len(blocks), width, 1.0 / width, first),
        out_shape=out,
        in_specs=[pl.BlockSpec(memory_space=pltpu.VMEM)] * len(operands),
        out_specs=pl.BlockSpec(memory_space=pltpu.VMEM),
        compiler_params=pltpu.CompilerParams(vmem_limit_bytes=4 << 20),
        cost_estimate=pl.CostEstimate(flops=1, bytes_accessed=1, transcendentals=0),
    )(*operands)


def on_device(resident_act, resident_grad, source_act, source_grad, probes):
    blocks = lax.axis_size("blk")
    source_total = source_act.shape[1] * blocks * lax.axis_size("src")
    res_act, res_grad = resident_act[0], resident_grad[0]

    own = jnp.concatenate([source_act[0], source_grad[0], probes], axis=1)
    tags = [None]
    for _ in range(len(TOUCH_AFTER)):
        tags.append(touch(res_act, res_grad, tags[-1]))
    held = {(0, 0): own}
    order = [(0, 0)]
    for hop, offset in ROUTE:
        there = moved(offset, hop)
        held[there] = lax.ppermute(held[offset], "blk", hop_pairs(hop))
        order.append(there)
    total = None
    begin = 0
    for index, size in enumerate(CHUNKS):
        total = add_chunk(total, tags[-1] if index == len(CHUNKS) - 1 else tags[1], res_act, res_grad, [held[o] for o in order[begin : begin + size]])
        begin += size

    layer = lax.axis_index("layer")
    core, high = layer % 2, layer // 2
    pieces = total.reshape(2, 2, -1, total.shape[1])
    keep = lax.dynamic_index_in_dim(pieces, core, 1, keepdims=False)
    give = lax.dynamic_index_in_dim(pieces, 1 - core, 1, keepdims=False)
    chip = keep + lax.ppermute(give, "layer", [(l, l ^ 1) for l in range(LAYERS)])
    mine = lax.dynamic_index_in_dim(chip, high, 0, keepdims=False)
    other = lax.dynamic_index_in_dim(chip, 1 - high, 0, keepdims=False).astype(jnp.bfloat16)

    def exchange(value, flip_src, flip_high):
        pairs = [
            (s * LAYERS + l, (s ^ flip_src) * LAYERS + (l ^ (2 * flip_high)))
            for s in range(2)
            for l in range(LAYERS)
        ]
        return lax.ppermute(value, ("src", "layer"), pairs)

    far = exchange(other, 0, 1)
    wrap = exchange(other, 1, 1)
    near = exchange(mine.astype(jnp.bfloat16), 1, 0)
    result = mine + near.astype(jnp.float32) + wrap.astype(jnp.float32) + far.astype(jnp.float32)
    return result * jnp.float32((LAYERS * source_total) ** (-0.5))


def solution(mesh):
    in_specs = (
        P("layer", "blk", None),
        P("layer", "blk", None),
        P("layer", ("blk", "src"), None),
        P("layer", ("blk", "src"), None),
        P(("blk", "src"), None),
    )
    out_specs = P(("blk", "layer"), None)
    return jax.shard_map(
        on_device, mesh=mesh, in_specs=in_specs, out_specs=out_specs, check_vma=False
    )
```
